32 devices in a mesh: dp: 16 (over z, y, x), tensor: 2 (over core).
Axes of the slice: x: 2, y: 2, z: 4, core: 2. Of those that a mesh axis runs over, the one named last changes fastest.
Arguments:
- block_input: bfloat16 [4096, 1536], P('dp'), may hold values from -6 to 6
- norm_gain: float32 [2, 1536], replicated, may hold values from 0.5 to 1.5
- zx_weight: bfloat16 [2, 1536, 2, 3072], P(None, None, None, 'tensor'), may hold values from -0.15625 to 0.15625
- bc_weight: bfloat16 [2, 1536, 256], replicated, may hold values from -0.15625 to 0.15625
- dt_weight: bfloat16 [2, 1536, 48], P(None, None, 'tensor'), may hold values from -0.15625 to 0.15625
- conv_x: float32 [2, 5, 3072], P(None, None, 'tensor'), may hold values from -0.5 to 0.5
- conv_bc: float32 [2, 5, 256], replicated, may hold values from -0.5 to 0.5
- head_params: float32 [2, 3, 48], P(None, None, 'tensor'), may hold values from -7 to 2
- gate_gain: float32 [2, 3072], P(None, 'tensor'), may hold values from 0.5 to 1.5
- out_weight: bfloat16 [2, 3072, 1536], P(None, 'tensor'), may hold values from -0.109375 to 0.109375
- seq_lengths: int32 [4], replicated, may hold values from 1 to 2176, 4096 in all
- out_cotangent: bfloat16 [4096, 1536], P('dp'), may hold values from -6 to 6
Outputs:
- block_output: bfloat16 [4096, 1536], P('dp')
- input_grad: float32 [4096, 1536], P('dp')
- norm_gain_grad: float32 [2, 1536], replicated
- zx_weight_grad: float32 [2, 1536, 2, 3072], P(None, 'dp', None, 'tensor')
- bc_weight_grad: float32 [2, 1536, 256], P(None, 'dp')
- dt_weight_grad: float32 [2, 1536, 48], P(None, 'dp', 'tensor')
- conv_x_grad: float32 [2, 5, 3072], P(None, None, 'tensor')
- conv_bc_grad: float32 [2, 5, 256], replicated
- head_params_grad: float32 [2, 3, 48], P(None, None, 'tensor')
- gate_gain_grad: float32 [2, 3072], P(None, 'tensor')
- out_weight_grad: float32 [2, 3072, 1536], P(None, 'tensor', 'dp')
The draws below stay inside these ranges and needn't reach their ends.
Inputs may be any that keep to these rules, and one draw needn't show every extreme that they name: `seq_lengths`: the lengths sum to 4096 and the longest is exactly 2176.
All inputs are finite; a program needn't handle non-finite values.
Results may differ from the reference program's by a relative error of at most 0.012.
The reference program's roundings to bfloat16 on the way count: a program that leaves them out, or rounds other values in their place, can miss the bound.
Values sent between devices are 32-bit elements; how exact they have to be, the bound alone decides.
A program may use at most 320 MiB of HBM per device.

```python
import math
import jax
import jax.numpy as jnp
import numpy as np
from jax import lax

D = 1536
HEADS = 48
HEAD_DIM = 64
STATE = 128
CONV = 4
GROUP = 256
LAYERS = 2
INNER = 3072
TOKENS = 4096
SEQS = 4
MAXLEN = 2176


def draw_head_params(key, part):
    subkeys = jax.random.split(key, 3)
    shape = (LAYERS, 1, HEADS)
    bias_row = jax.random.uniform(subkeys[0], shape, jnp.float32, -5.5, -3.5)
    decay_row = jax.random.uniform(subkeys[1], shape, jnp.float32, -6.0, 2.0)
    skip_row = jax.random.uniform(subkeys[2], shape, jnp.float32, 0.5, 1.5)
    return jnp.concatenate([bias_row, decay_row, skip_row], axis=1)


def level_of(key, shape, shards, low, high):
    level, own = 1.0, jax.random.fold_in(key, 6)
    for dim, shards_of in shards:
        draws = jnp.exp(jax.random.uniform(jax.random.fold_in(own, dim), (shards_of,), jnp.float32, low / len(shards), high / len(shards)))
        level = level * jnp.repeat(draws, shape[dim] // shards_of).reshape([-1 if axis == dim else 1 for axis in range(len(shape))])
    return level


def profile(count, total, reach, lean):
    loads = [(1 << 20) // math.isqrt(rank ** lean) + 1 for rank in range(2, count + 1)]
    rest, counts = total - reach - (count - 1), [1] * (count - 1)
    while rest > 0:
        movable = [i for i in range(count - 1) if counts[i] < reach]
        pool, remaining = sum([loads[i] for i in movable]), rest
        for i in movable:
            extra = min(reach - counts[i], max(1, remaining * loads[i] // pool), rest)
            counts[i] = counts[i] + extra
            rest = rest - extra
    return np.array([reach] + counts)


def uneven_parts(stream_key, number_of, total, reach, lean):
    if number_of == 2:
        one = jax.random.randint(stream_key, (), max(1, total - reach), min(reach, total - 1) + 1)
        return jnp.stack([one, total - one])
    lengths = jnp.asarray(profile(number_of, total, reach, lean), jnp.int32)
    pairs = (number_of - 1) // 2
    source_of, sink = lengths[1:1 + 2 * pairs:2], lengths[2:2 + 2 * pairs:2]
    room = jnp.minimum(source_of - 1, reach - sink)
    shifted = jax.random.randint(jax.random.fold_in(stream_key, 1), (pairs,), 0, 1 << 20) % (room + 1)
    lengths = lengths.at[1:1 + 2 * pairs:2].set(source_of - shifted).at[2:2 + 2 * pairs:2].set(sink + shifted)
    return lengths[jax.random.permutation(jax.random.fold_in(stream_key, 2), number_of)]


def gaussian(stream_key, extent, scale, reach, pieces=(), kind=jnp.bfloat16):
    entries = scale * jax.random.normal(stream_key, extent, jnp.float32)
    if pieces:
        entries = entries * level_of(stream_key, extent, pieces, -0.22, 0.18)
    return jnp.clip(entries, -reach, reach).astype(kind)


def setup_inputs(seed: int = 0) -> dict:
    arg_keys = jax.random.split(jax.random.key(seed), 13)
    block_input = gaussian(arg_keys[0], (TOKENS, D), 1.0, 6.0, ((0, 16),))
    norm_gain = jnp.clip(1.0 + 0.1 * jax.random.normal(arg_keys[1], (LAYERS, D), jnp.float32), 0.5, 1.5)
    zx_weight = gaussian(arg_keys[2], (LAYERS, D, 2, INNER), D ** -0.5, 0.15625, ((3, 2),))
    bc_weight = gaussian(arg_keys[3], (LAYERS, D, 2 * STATE), D ** -0.5, 0.15625)
    dt_weight = gaussian(arg_keys[4], (LAYERS, D, HEADS), D ** -0.5, 0.15625, ((2, 2),))
    conv_x = jnp.clip(jax.random.uniform(arg_keys[5], (LAYERS, CONV + 1, INNER), jnp.float32, -0.5, 0.5) * level_of(arg_keys[5], (LAYERS, CONV + 1, INNER), ((2, 2),), -0.4, 0.0), -0.5, 0.5)
    conv_bc = jnp.clip(jax.random.uniform(arg_keys[6], (LAYERS, CONV + 1, 2 * STATE), jnp.float32, -0.5, 0.5), -0.5, 0.5)
    head_params = draw_head_params(jax.random.fold_in(arg_keys[12], 71), 0)
    gate_gain = jnp.clip(1.0 + 0.1 * jax.random.normal(arg_keys[8], (LAYERS, INNER), jnp.float32), 0.5, 1.5)
    out_weight = gaussian(arg_keys[9], (LAYERS, INNER, D), INNER ** -0.5, 0.109375, ((1, 2),))
    seq_lengths = uneven_parts(arg_keys[10], SEQS, TOKENS, MAXLEN, 2).astype(jnp.int32)
    out_cotangent = gaussian(arg_keys[11], (TOKENS, D), 1.0, 6.0, ((0, 16),))
    return {"block_input": block_input, "norm_gain": norm_gain, "zx_weight": zx_weight, "bc_weight": bc_weight, "dt_weight": dt_weight, "conv_x": conv_x, "conv_bc": conv_bc, "head_params": head_params, "gate_gain": gate_gain, "out_weight": out_weight, "seq_lengths": seq_lengths, "out_cotangent": out_cotangent}


epsilon = 1e-05

def segment_of(positions, seq_ends):
    counted = lax.optimization_barrier(jnp.sum((seq_ends[None, :] <= positions[:, None]).astype(jnp.int32), axis=1))
    return jnp.where(positions < 0, -1, counted).astype(jnp.int32)

def rms_scale(hidden, gain):
    mean_sq = lax.optimization_barrier(jnp.mean(hidden * hidden, axis=1, keepdims=True))
    return hidden * lax.rsqrt(mean_sq + epsilon) * gain

def conv_silu(pre_ext, seg_ext, tap_rows):
    count = pre_ext.shape[0] - (CONV - 1)
    current = seg_ext[CONV - 1:]
    total = jnp.zeros((count, pre_ext.shape[1]), jnp.float32) + tap_rows[CONV]
    for offset in range(CONV):
        same_seq = seg_ext[offset:offset + count] == current
        total = total + tap_rows[offset] * jnp.where(same_seq[:, None], pre_ext[offset:offset + count], 0.0)
    return jax.nn.silu(total)

def group_step(state_now, group_inputs):
    x_scaled, rate_block, b_block, c_block, seg_block, seg_prior = group_inputs
    cumulative = jnp.cumsum(rate_block, axis=0)
    length = seg_block.shape[0]
    lower_mask = jnp.arange(length)[:, None] >= jnp.arange(length)[None, :]
    same_mask = lower_mask & (seg_block[:, None] == seg_block[None, :])
    decayed = jnp.exp(jnp.where(same_mask[:, :, None], cumulative[:, None, :] - cumulative[None, :, :], -1e+30))
    intersection = jnp.dot(c_block, b_block.T, precision=lax.Precision.HIGHEST)
    outputs = jnp.einsum('ijh,jhp->ihp', decayed * intersection[:, :, None], x_scaled, precision=lax.Precision.HIGHEST)
    alive_rows = (seg_block == seg_prior).astype(jnp.float32)
    carried = jnp.einsum('in,hpn->ihp', c_block, state_now, precision=lax.Precision.HIGHEST)
    outputs = outputs + (alive_rows[:, None] * jnp.exp(cumulative))[:, :, None] * carried
    to_end = jnp.where((seg_block == seg_block[-1])[:, None], jnp.exp(cumulative[-1][None, :] - cumulative), 0.0)
    state_next = (alive_rows[-1] * jnp.exp(cumulative[-1]))[:, None, None] * state_now
    state_next = state_next + jnp.einsum('jh,jhp,jn->hpn', to_end, x_scaled, b_block, precision=lax.Precision.HIGHEST)
    return (state_next, outputs)

def local_scan(x_act, dt_raw, bc_act, params, segments, seg_before, start_state):
    count = x_act.shape[0]
    heads = params.shape[1]
    width = x_act.shape[1] // heads
    half = bc_act.shape[1] // 2
    step_size = jax.nn.softplus(dt_raw + params[0])
    rate = -jnp.exp(params[1]) * step_size
    x_heads = x_act.reshape(count, heads, width)
    x_scaled = x_heads * step_size[:, :, None]
    blocks = count // GROUP
    group_inputs = (x_scaled.reshape(blocks, GROUP, heads, width), rate.reshape(blocks, GROUP, heads), bc_act[:, :half].reshape(blocks, GROUP, half), bc_act[:, half:].reshape(blocks, GROUP, half), segments.reshape(blocks, GROUP), seg_before)
    final_state, outputs = lax.scan(jax.checkpoint(group_step), start_state, group_inputs)
    return (outputs.reshape(count, heads, width) + params[2][None, :, None] * x_heads, final_state, rate)

def middle(gate_in, x_pre, bc_pre, dt_raw, taps_x, taps_bc, params, gain, seg_ext, segments, seg_before):
    count = x_pre.shape[0]
    x_ext = jnp.concatenate([jnp.zeros((CONV - 1, x_pre.shape[1]), jnp.float32), x_pre], 0)
    bc_ext = jnp.concatenate([jnp.zeros((CONV - 1, bc_pre.shape[1]), jnp.float32), bc_pre], 0)
    x_act = conv_silu(x_ext, seg_ext, taps_x)
    bc_act = conv_silu(bc_ext, seg_ext, taps_bc)
    start_state = jnp.zeros((HEADS, HEAD_DIM, STATE), jnp.float32)
    outputs, final_state, rate = local_scan(x_act, dt_raw, bc_act, params, segments, seg_before, start_state)
    gated = outputs.reshape(count, INNER) * jax.nn.silu(gate_in)
    scale = lax.rsqrt(lax.optimization_barrier(jnp.mean(gated * gated, axis=1, keepdims=True)) + epsilon)
    return gated * scale * gain

def project(hidden, gain, w_zx, w_bc, w_dt):
    normed_bf = rms_scale(hidden, gain).astype(jnp.bfloat16)
    projected = jnp.dot(normed_bf, w_zx, preferred_element_type=jnp.float32)
    bc_pre = jnp.dot(normed_bf, w_bc, preferred_element_type=jnp.float32)
    dt_raw = jnp.dot(normed_bf, w_dt, preferred_element_type=jnp.float32)
    return (normed_bf, projected[:, :INNER], projected[:, INNER:], bc_pre, dt_raw)

def reference(block_input, norm_gain, zx_weight, bc_weight, dt_weight, conv_x, conv_bc, head_params, gate_gain, out_weight, seq_lengths, out_cotangent):
    seq_ends = jnp.cumsum(seq_lengths).astype(jnp.int32)
    segments = segment_of(jnp.arange(TOKENS, dtype=jnp.int32), seq_ends)
    seg_ext = segment_of(jnp.arange(-(CONV - 1), TOKENS, dtype=jnp.int32), seq_ends)
    seg_before = segment_of(jnp.arange(TOKENS // GROUP, dtype=jnp.int32) * GROUP - 1, seq_ends)

    def middle_fn(gate_in, x_pre, bc_pre, dt_raw, taps_x, taps_bc, params, gain):
        return middle(gate_in, x_pre, bc_pre, dt_raw, taps_x, taps_bc, params, gain, seg_ext, segments, seg_before)
    hidden = block_input.astype(jnp.float32)
    saved = []
    for layer_index in range(LAYERS):
        saved.append(hidden)
        w_zx = zx_weight[layer_index].reshape(D, 2 * INNER)
        normed_bf, gate_in, x_pre, bc_pre, dt_raw = project(hidden, norm_gain[layer_index], w_zx, bc_weight[layer_index], dt_weight[layer_index])
        mixed = middle_fn(gate_in, x_pre, bc_pre, dt_raw, conv_x[layer_index], conv_bc[layer_index], head_params[layer_index], gate_gain[layer_index]).astype(jnp.bfloat16)
        hidden = hidden + jnp.dot(mixed, out_weight[layer_index], preferred_element_type=jnp.float32)
    block_output = hidden.astype(jnp.bfloat16)
    grad = out_cotangent.astype(jnp.float32)
    results = [[] for index in range(9)]
    for layer_index in reversed(range(LAYERS)):
        hidden_in = saved[layer_index]
        w_zx = zx_weight[layer_index].reshape(D, 2 * INNER)
        normed_bf, gate_in, x_pre, bc_pre, dt_raw = project(hidden_in, norm_gain[layer_index], w_zx, bc_weight[layer_index], dt_weight[layer_index])
        mixed_f, pull_mid = jax.vjp(middle_fn, gate_in, x_pre, bc_pre, dt_raw, conv_x[layer_index], conv_bc[layer_index], head_params[layer_index], gate_gain[layer_index])
        mixed = mixed_f.astype(jnp.bfloat16)
        grad_bf = grad.astype(jnp.bfloat16)
        d_out_w = jnp.dot(mixed.T, grad_bf, preferred_element_type=jnp.float32)
        d_mixed = jnp.dot(grad_bf, out_weight[layer_index].T, preferred_element_type=jnp.float32)
        d_z, d_xpre, d_bcpre, d_dtraw, d_cx, d_cbc, d_params, d_gate = pull_mid(d_mixed)
        d_proj = jnp.concatenate([d_z, d_xpre], 1).astype(jnp.bfloat16)
        d_bc_bf = d_bcpre.astype(jnp.bfloat16)
        d_dt_bf = d_dtraw.astype(jnp.bfloat16)
        d_zx_w = jnp.dot(normed_bf.T, d_proj, preferred_element_type=jnp.float32).reshape(D, 2, INNER)
        d_bc_w = jnp.dot(normed_bf.T, d_bc_bf, preferred_element_type=jnp.float32)
        d_dt_w = jnp.dot(normed_bf.T, d_dt_bf, preferred_element_type=jnp.float32)
        d_normed = jnp.dot(d_proj, w_zx.T, preferred_element_type=jnp.float32) + jnp.dot(d_bc_bf, bc_weight[layer_index].T, preferred_element_type=jnp.float32) + jnp.dot(d_dt_bf, dt_weight[layer_index].T, preferred_element_type=jnp.float32)
        unused, pull_norm = jax.vjp(rms_scale, hidden_in, norm_gain[layer_index])
        d_hidden, d_gain = pull_norm(d_normed)
        grad = grad + d_hidden
        for slot, value in enumerate([d_gain, d_zx_w, d_bc_w, d_dt_w, d_cx, d_cbc, d_params, d_gate, d_out_w]):
            results[slot].insert(0, value)
    stacked = [jnp.stack(entry, 0) for entry in results]
    return (block_output, grad, stacked[0], stacked[1], stacked[2], stacked[3], stacked[4], stacked[5], stacked[6], stacked[7], stacked[8])
```

```python
import functools

import jax
import jax.numpy as jnp
from jax import lax
from jax.experimental import pallas as pl
from jax.experimental.pallas import tpu as pltpu
from jax.sharding import PartitionSpec as P

D = 1536
CONV = 4
GROUP = 256
LAYERS = 2
INNER = 3072
PLANE = 4


epsilon = 1e-05


def shifted(array, axis, by):
    size = lax.axis_size(axis)
    pairs = [(i, i + by) for i in range(size) if 0 <= i + by < size]
    return lax.ppermute(array, axis, pairs)


def state_kernel(reverse, planes, f_ref, t_ref, o_ref, gath, tg, zin, zout, back, s_a, r_a, s_t, r_t, s_z, r_z, s_b, r_b):
    me = lax.axis_index("dp")
    i = lax.rem(me, PLANE)
    q = me // PLANE
    per = zin.shape[0]
    at = planes - 1 - q if reverse else q
    ahead = me - PLANE if reverse else me + PLANE
    behind = me + PLANE if reverse else me - PLANE
    order = tuple(reversed(range(PLANE))) if reverse else tuple(range(PLANE))

    def send(src, dst, ss, rs, to):
        return pltpu.make_async_remote_copy(
            src_ref=src, dst_ref=dst, send_sem=ss, recv_sem=rs, device_id={"dp": to}, device_id_type=pl.DeviceIdType.MESH
        )

    barrier = pltpu.get_barrier_semaphore()
    peers = [lax.rem(i + k, PLANE) for k in range(1, PLANE)]
    for peer in peers:
        pl.semaphore_signal(
            barrier, inc=1, device_id={"dp": q * PLANE + peer}, device_id_type=pl.DeviceIdType.MESH
        )

    @pl.when(at > 0)
    def _():
        pl.semaphore_signal(barrier, inc=1, device_id={"dp": behind}, device_id_type=pl.DeviceIdType.MESH)

    @pl.when(at < planes - 1)
    def _():
        pl.semaphore_signal(barrier, inc=1, device_id={"dp": ahead}, device_id_type=pl.DeviceIdType.MESH)

    chain = jnp.where(at > 0, 1, 0) + jnp.where(at < planes - 1, 1, 0)
    pl.semaphore_wait(barrier, PLANE - 1 + chain)

    t_copies = [
        send(t_ref.at[peer], tg.at[i], s_t.at[k], r_t.at[k], q * PLANE + peer) for k, peer in enumerate(peers)
    ]
    for copy in t_copies:
        copy.start()
    a_copies = [
        [
            send(f_ref.at[peer * per + r], gath.at[i, r], s_a.at[r, k], r_a.at[r, k], q * PLANE + peer)
            for k, peer in enumerate(peers)
        ]
        for r in range(per)
    ]
    for row in a_copies:
        for copy in row:
            copy.start()
    tg[i] = t_ref[i]
    for r in range(per):
        gath[i, r] = f_ref[i * per + r]
    for copy in t_copies:
        copy.wait_recv()
    z_copies = [send(zout.at[r], zin.at[r], s_z.at[r], r_z.at[r], ahead) for r in range(per)]
    b_copies = []
    for r in range(per):
        for copy in a_copies[r]:
            copy.wait_recv()

        @pl.when(at == 0)
        def _(r=r):
            zin[r] = jnp.zeros_like(zin[r])

        through = [tg[j, pl.ds(r, 1), :] for j in order]
        states = [gath[j, r] for j in order]
        total = states[0]
        decay = through[0]
        for j in range(1, PLANE):
            total = states[j] + through[j] * total
            decay = decay * through[j]

        @pl.when(at > 0)
        def _(r=r):
            z_copies[r].wait_recv()

        inc = zin[r]
        zout[r] = total + decay * inc

        @pl.when(at < planes - 1)
        def _(r=r):
            z_copies[r].start()

        for j in range(PLANE):
            back[order[j], r] = inc
            inc = states[j] + through[j] * inc
        o_ref[i * per + r] = back[i, r]
        row = [
            send(back.at[peer, r], o_ref.at[i * per + r], s_b.at[r, k], r_b.at[r, k], q * PLANE + peer)
            for k, peer in enumerate(peers)
        ]
        for copy in row:
            copy.start()
        b_copies.append(row)
    for copy in t_copies:
        copy.wait_send()
    for r in range(per):
        for copy in a_copies[r]:
            copy.wait_send()
        for copy in b_copies[r]:
            copy.wait()

        @pl.when(at < planes - 1)
        def _(r=r):
            z_copies[r].wait_send()


def entering(through, state, reverse, call):
    heads, width, depth = state.shape
    planes = lax.axis_size("dp") // PLANE
    per = heads // PLANE
    rows = -(-per // 8) * 8
    spread = jnp.pad(through.reshape(PLANE, per), ((0, 0), (0, rows - per)))
    spread = jnp.broadcast_to(spread[:, :, None], (PLANE, rows, depth))
    f32 = jnp.float32
    dma = pltpu.SemaphoreType.DMA
    vmem = pl.BlockSpec(memory_space=pltpu.VMEM)
    return pl.pallas_call(
        functools.partial(state_kernel, reverse, planes),
        out_shape=jax.ShapeDtypeStruct(state.shape, f32),
        in_specs=[vmem, vmem],
        out_specs=vmem,
        scratch_shapes=[
            pltpu.VMEM((PLANE, per, width, depth), f32),
            pltpu.VMEM((PLANE, rows, depth), f32),
            pltpu.VMEM((per, width, depth), f32),
            pltpu.VMEM((per, width, depth), f32),
            pltpu.VMEM((PLANE, per, width, depth), f32),
            dma((per, PLANE - 1)),
            dma((per, PLANE - 1)),
            dma((PLANE - 1,)),
            dma((PLANE - 1,)),
            dma((per,)),
            dma((per,)),
            dma((per, PLANE - 1)),
            dma((per, PLANE - 1)),
        ],
        compiler_params=pltpu.CompilerParams(collective_id=call, has_side_effects=True),
        name="state_chain",
    )(state, spread)


def segment_of(positions, seq_ends):
    counted = jnp.sum((seq_ends[None, :] <= positions[:, None]).astype(jnp.int32), axis=1)
    return jnp.where(positions < 0, -1, counted)


def rms_scale(hidden, gain):
    mean_sq = jnp.mean(hidden * hidden, axis=1, keepdims=True)
    return hidden * lax.rsqrt(mean_sq + epsilon) * gain


def conv_silu(pre_ext, seg_ext, tap_rows):
    count = pre_ext.shape[0] - (CONV - 1)
    current = seg_ext[CONV - 1 :]
    total = jnp.zeros((count, pre_ext.shape[1]), jnp.float32) + tap_rows[CONV]
    for offset in range(CONV):
        same_seq = seg_ext[offset : offset + count] == current
        total = total + tap_rows[offset] * jnp.where(
            same_seq[:, None], pre_ext[offset : offset + count], 0.0
        )
    return jax.nn.silu(total)


def group_step(state_now, group_inputs):
    x_scaled, rate_block, b_block, c_block, seg_block, seg_prior = group_inputs
    cumulative = jnp.cumsum(rate_block, axis=0)
    length = seg_block.shape[0]
    lower_mask = jnp.arange(length)[:, None] >= jnp.arange(length)[None, :]
    same_mask = lower_mask & (seg_block[:, None] == seg_block[None, :])
    decayed = jnp.exp(
        jnp.where(same_mask[:, :, None], cumulative[:, None, :] - cumulative[None, :, :], -1e30)
    )
    intersection = jnp.dot(c_block, b_block.T, precision=lax.Precision.HIGHEST)
    outputs = jnp.einsum(
        "ijh,jhp->ihp",
        decayed * intersection[:, :, None],
        x_scaled,
        precision=lax.Precision.HIGHEST,
    )
    alive_rows = (seg_block == seg_prior).astype(jnp.float32)
    carried = jnp.einsum("in,hpn->ihp", c_block, state_now, precision=lax.Precision.HIGHEST)
    outputs = outputs + (alive_rows[:, None] * jnp.exp(cumulative))[:, :, None] * carried
    to_end = jnp.where(
        (seg_block == seg_block[-1])[:, None], jnp.exp(cumulative[-1][None, :] - cumulative), 0.0
    )
    state_next = (alive_rows[-1] * jnp.exp(cumulative[-1]))[:, None, None] * state_now
    state_next = state_next + jnp.einsum(
        "jh,jhp,jn->hpn", to_end, x_scaled, b_block, precision=lax.Precision.HIGHEST
    )
    return (state_next, outputs)


def local_scan(x_act, dt_raw, bc_act, params, segments, seg_before, start_state):
    count = x_act.shape[0]
    heads = params.shape[1]
    width = x_act.shape[1] // heads
    half = bc_act.shape[1] // 2
    step_size = jax.nn.softplus(dt_raw + params[0])
    rate = -jnp.exp(params[1]) * step_size
    x_heads = x_act.reshape(count, heads, width)
    x_scaled = x_heads * step_size[:, :, None]
    blocks = count // GROUP
    group_inputs = (
        x_scaled.reshape(blocks, GROUP, heads, width),
        rate.reshape(blocks, GROUP, heads),
        bc_act[:, :half].reshape(blocks, GROUP, half),
        bc_act[:, half:].reshape(blocks, GROUP, half),
        segments.reshape(blocks, GROUP),
        seg_before,
    )
    final_state, outputs = lax.scan(group_step, start_state, group_inputs)
    return (
        outputs.reshape(count, heads, width) + params[2][None, :, None] * x_heads,
        final_state,
        rate,
    )


def device_section(x_act, dt_raw, bc_act, params, segments, seg_before, seg_prior):
    heads = params.shape[1]
    half = bc_act.shape[1] // 2
    start_state = jnp.zeros((heads, x_act.shape[1] // heads, half), jnp.float32)
    outputs, final_state, rate = local_scan(
        x_act, dt_raw, bc_act, params, segments, seg_before, start_state
    )
    cumulative = jnp.cumsum(rate, axis=0)
    through = (segments[-1] == seg_prior).astype(jnp.float32)
    return (outputs, final_state, through * jnp.exp(cumulative[-1]), cumulative, bc_act[:, half:])


def state_input(incoming, cumulative, c_matrix, alive_rows):
    weights = alive_rows[:, None] * jnp.exp(cumulative)
    return weights[:, :, None] * jnp.einsum(
        "tn,hpn->thp", c_matrix, incoming, precision=lax.Precision.HIGHEST
    )


def contract_rows(left, right):
    return lax.dot_general(
        left.astype(jnp.bfloat16), right.astype(jnp.bfloat16), (((0,), (0,)), ((), ())), preferred_element_type=jnp.float32
    )


def contract_cols(left, right):
    return lax.dot_general(
        left, right, (((1,), (1,)), ((), ())), preferred_element_type=jnp.float32
    )


def swapped(array):
    return lax.ppermute(array, "tensor", [(0, 1), (1, 0)])


def pair_sum(array):
    return array + swapped(array)


def from_plane(array, k):
    size = lax.axis_size("dp")
    return lax.ppermute(array, "dp", [(d, d ^ k) for d in range(size)])


def plane_gather(rows):
    core = lax.axis_index("tensor")
    half = rows.shape[1] // 2
    mine = lax.dynamic_slice_in_dim(rows, core * half, half, 1)
    mine = jnp.concatenate([mine] + [from_plane(mine, k) for k in range(1, PLANE)], 0)
    other = swapped(mine)
    first = jnp.where(core == 0, mine, other)
    second = jnp.where(core == 0, other, mine)
    return jnp.concatenate([first, second], 1)


def plane_exchange(parts):
    place = lax.rem(lax.axis_index("dp"), PLANE)
    take = lambda k: lax.dynamic_index_in_dim(parts, place ^ k, 0, keepdims=False)
    return jnp.concatenate([take(0)] + [from_plane(take(k), k) for k in range(1, PLANE)], 0)


def columns_of(array, pad=0):
    rows, columns = array.shape
    parts = array.reshape(rows, PLANE, columns // PLANE).transpose(1, 0, 2)
    return jnp.pad(parts, ((0, 0), (0, 0), (0, pad)))


def plane_sums(all_left, all_right, unit):
    size = lax.axis_size("dp")
    part = contract_rows(all_left * unit, all_right * unit)
    groups = [[q * PLANE + i for q in range(size // PLANE)] for i in range(PLANE)]
    return lax.psum_scatter(part, "dp", scatter_dimension=0, axis_index_groups=groups, tiled=True)


def hand_back(sums):
    place = lax.rem(lax.axis_index("dp"), PLANE)
    rows = sums.shape[0] // PLANE
    got = plane_exchange(sums.reshape(PLANE, rows, -1)).reshape(PLANE, rows, -1)
    return jnp.stack([lax.dynamic_index_in_dim(got, place ^ k, 0, keepdims=False) for k in range(PLANE)], 0)


def per_device(
    block_input,
    norm_gain,
    zx_weight,
    bc_weight,
    dt_weight,
    conv_x,
    conv_bc,
    head_params,
    gate_gain,
    out_weight,
    seq_lengths,
    out_cotangent,
):
    token_rows = block_input.shape[0]
    inner_local = out_weight.shape[1]
    heads_local = head_params.shape[2]
    bc_columns = bc_weight.shape[2]
    tail_rows = CONV - 1
    split_at = token_rows - tail_rows
    seq_ends = jnp.cumsum(seq_lengths)
    first_pos = lax.axis_index("dp") * token_rows
    segments = segment_of(first_pos + jnp.arange(token_rows, dtype=jnp.int32), seq_ends)
    seg_ext = segment_of(first_pos + jnp.arange(-tail_rows, token_rows, dtype=jnp.int32), seq_ends)
    seg_before = segment_of(
        first_pos + jnp.arange(token_rows // GROUP, dtype=jnp.int32) * GROUP - 1, seq_ends
    )
    seg_prior = seg_before[0]
    unit = (seq_lengths[0] > 0).astype(jnp.float32)
    alive_rows = (segments == seg_prior).astype(jnp.float32)

    def section_fn(x_act, dt_raw, bc_act, params):
        return device_section(x_act, dt_raw, bc_act, params, segments, seg_before, seg_prior)

    def state_fn(incoming, cumulative, c_matrix):
        return state_input(incoming, cumulative, c_matrix, alive_rows)

    def conv_fn(pre_ext, tap_rows):
        return conv_silu(pre_ext, seg_ext, tap_rows)

    hidden = block_input.astype(jnp.float32)
    kept = []
    for layer_index in range(LAYERS):
        w_zx = zx_weight[layer_index].reshape(D, 2 * inner_local)
        normed_f, pull_norm = jax.vjp(rms_scale, hidden, norm_gain[layer_index])
        normed_bf = normed_f.astype(jnp.bfloat16)
        normed_all = plane_gather(normed_f)
        projected = jnp.dot(normed_bf, w_zx, preferred_element_type=jnp.float32)
        gate_in = projected[:, :inner_local]
        x_pre = projected[:, inner_local:]
        bc_pre = jnp.dot(normed_bf, bc_weight[layer_index], preferred_element_type=jnp.float32)
        dt_raw = jnp.dot(normed_bf, dt_weight[layer_index], preferred_element_type=jnp.float32)
        tails = shifted((x_pre[split_at:], bc_pre[split_at:]), "dp", 1)
        x_ext = jnp.concatenate([tails[0], x_pre], 0)
        bc_ext = jnp.concatenate([tails[1], bc_pre], 0)
        x_act, pull_cx = jax.vjp(conv_fn, x_ext, conv_x[layer_index])
        bc_act, pull_cbc = jax.vjp(conv_fn, bc_ext, conv_bc[layer_index])
        section_out, pull_section = jax.vjp(
            section_fn, x_act, dt_raw, bc_act, head_params[layer_index]
        )
        outputs, final_state, through, cumulative, c_matrix = section_out
        incoming = entering(through, final_state, False, layer_index)
        from_state, pull_state = jax.vjp(state_fn, incoming, cumulative, c_matrix)
        ssd_out = (outputs + from_state).reshape(token_rows, inner_local)
        gated = ssd_out * jax.nn.silu(gate_in)
        squares = pair_sum(jnp.sum(gated * gated, axis=1))
        scale = lax.rsqrt(squares / INNER + epsilon)
        mixed_f = gated * scale[:, None] * gate_gain[layer_index]
        mixed = mixed_f.astype(jnp.bfloat16)
        mixed_parts = plane_exchange(columns_of(mixed_f))
        out_sum = pair_sum(jnp.dot(mixed, out_weight[layer_index], preferred_element_type=jnp.float32))
        kept.append(
            (
                pull_norm,
                normed_all,
                gate_in,
                ssd_out,
                gated,
                scale,
                mixed_parts,
                pull_cx,
                pull_cbc,
                pull_section,
                pull_state,
                incoming,
                through,
            )
        )
        hidden = hidden + out_sum
    block_output = hidden.astype(jnp.bfloat16)
    grad = out_cotangent.astype(jnp.float32)
    large_list = []
    small_list = []
    for layer_index in reversed(range(LAYERS)):
        (
            pull_norm,
            normed_all,
            gate_in,
            ssd_out,
            gated,
            scale,
            mixed_parts,
            pull_cx,
            pull_cbc,
            pull_section,
            pull_state,
            incoming,
            through,
        ) = kept[layer_index]
        grad_bf = grad.astype(jnp.bfloat16)
        grad_all = plane_gather(grad)
        d_out_w = plane_sums(grad_all, mixed_parts, unit)
        d_mixed = contract_cols(grad_bf, out_weight[layer_index])
        gain_row = gate_gain[layer_index]
        d_gate_gain = jnp.sum(d_mixed * gated * scale[:, None], axis=0)
        dotted = pair_sum(jnp.sum(d_mixed * gain_row * gated, axis=1))
        d_gated = (
            scale[:, None] * gain_row * d_mixed
            - gated * (scale * scale * scale * dotted / INNER)[:, None]
        )
        sigma = jax.nn.sigmoid(gate_in)
        d_ssd = d_gated * gate_in * sigma
        d_z = d_gated * ssd_out * sigma * (1.0 + gate_in * (1.0 - sigma))
        d_heads = d_ssd.reshape(token_rows, heads_local, -1)
        d_incoming, d_cumul, d_cmatrix = pull_state(d_heads)
        d_final = entering(through, d_incoming, True, LAYERS + layer_index)
        d_through = jnp.sum(d_final * incoming, axis=(1, 2))
        d_xact, d_dtraw, d_bcact, d_params = pull_section(
            (d_heads, d_final, d_through, d_cumul, d_cmatrix)
        )
        d_bcact = pair_sum(d_bcact)
        d_xext, d_cx = pull_cx(d_xact)
        d_bcext, d_cbc = pull_cbc(d_bcact)
        back = shifted((d_xext[:tail_rows], d_bcext[:tail_rows]), "dp", -1)
        d_xcore = d_xext[tail_rows:]
        d_bccore = d_bcext[tail_rows:]
        d_xpre = jnp.concatenate([d_xcore[:split_at], d_xcore[split_at:] + back[0]], 0)
        d_bcpre = jnp.concatenate([d_bccore[:split_at], d_bccore[split_at:] + back[1]], 0)
        d_proj_f = jnp.concatenate([d_z, d_xpre], 1)
        d_proj = d_proj_f.astype(jnp.bfloat16)
        d_bc_bf = d_bcpre.astype(jnp.bfloat16)
        d_dt_bf = d_dtraw.astype(jnp.bfloat16)
        w_zx = zx_weight[layer_index].reshape(D, 2 * inner_local)
        small_pad = -(bc_columns + heads_local) // PLANE % 128
        parts = jnp.concatenate(
            [
                columns_of(d_proj_f),
                columns_of(d_bcpre),
                columns_of(d_dtraw, small_pad),
            ],
            2,
        )
        d_in_w = plane_sums(normed_all, plane_exchange(parts), unit)
        head_part = contract_cols(d_proj, w_zx) + contract_cols(d_dt_bf, dt_weight[layer_index])
        d_normed = pair_sum(head_part) + contract_cols(d_bc_bf, bc_weight[layer_index])
        d_hidden, d_norm_gain = pull_norm(d_normed)
        grad = grad + d_hidden
        large_list.insert(0, (d_in_w, d_out_w))
        small_list.insert(0, (d_norm_gain, d_cx, d_cbc, d_params, d_gate_gain))

    def join(parts):
        return parts.transpose(1, 0, 2).reshape(parts.shape[1], -1)

    grads = []
    for d_in_w, d_out_w in large_list:
        got = hand_back(jnp.concatenate([d_in_w, d_out_w], 1))
        zx_end = 2 * inner_local // PLANE
        bc_end = zx_end + bc_columns // PLANE
        dt_end = bc_end + heads_local // PLANE
        grads.append(
            (
                join(got[:, :, :zx_end]).reshape(-1, 2, inner_local),
                join(got[:, :, zx_end:bc_end]),
                join(got[:, :, bc_end:dt_end]),
                join(got[:, :, d_in_w.shape[1] :]).T,
            )
        )
    large_sums = tuple(jnp.stack([entry[slot] for entry in grads], 0) for slot in range(4))
    small_stack = tuple((jnp.stack([entry[slot] for entry in small_list], 0) for slot in range(5)))
    small_sums = lax.psum(small_stack, "dp")
    return (
        block_output,
        grad,
        small_sums[0],
        large_sums[0],
        large_sums[1],
        large_sums[2],
        small_sums[1],
        small_sums[2],
        small_sums[3],
        small_sums[4],
        large_sums[3],
    )


def solution(mesh):
    placed = (
        P("dp", None),
        P(),
        P(None, None, None, "tensor"),
        P(),
        P(None, None, "tensor"),
        P(None, None, "tensor"),
        P(),
        P(None, None, "tensor"),
        P(None, "tensor"),
        P(None, "tensor", None),
        P(),
        P("dp", None),
    )
    return jax.shard_map(
        per_device,
        mesh=mesh,
        in_specs=placed,
        out_specs=(
            P("dp", None),
            P("dp", None),
            P(),
            P(None, "dp", None, "tensor"),
            P(None, "dp", None),
            P(None, "dp", "tensor"),
            P(None, None, "tensor"),
            P(),
            P(None, None, "tensor"),
            P(None, "tensor"),
            P(None, "tensor", "dp"),
        ),
        check_vma=False,
    )
```
